32 devices in a mesh: dp: 16 (over z, y, core), tensor: 2 (over x).
Axes of the slice: x: 2, y: 2, z: 4, core: 2. Of those that a mesh axis runs over, the one named last changes fastest.
Arguments:
- tokens: bfloat16 [21760, 1024], P('dp'), may hold values from -6 to 6
- d_out: bfloat16 [21760, 1024], P('dp'), may hold values from -6 to 6
- labels: int32 [32], replicated, may hold values from 0 to 999
- scale_ids: int32 [32, 680], P('dp'), may hold values from 0 to 9, never falling along the last dimension, each value on 1 to 256 neighbouring positions
- class_table: bfloat16 [1000, 1024], P(None, 'tensor'), may hold values from -6 to 6
- ada_weight: bfloat16 [1024, 6144], P(None, 'tensor'), may hold values from -0.1875 to 0.1875
- ada_bias: bfloat16 [6144], P('tensor'), may hold values from -3 to 3
- qkv_weight: bfloat16 [1024, 3, 1024], P(None, None, 'tensor'), may hold values from -0.1875 to 0.1875
- q_bias: bfloat16 [1024], P('tensor'), may hold values from -3 to 3
- v_bias: bfloat16 [1024], P('tensor'), may hold values from -3 to 3
- qk_scale: float32 [16], P('tensor'), may hold values from 2.3 to 3
- proj_weight: bfloat16 [1024, 1024], P('tensor'), may hold values from -0.75 to 0.75
- proj_bias: bfloat16 [1024], replicated, may hold values from -2 to 2
- fc1_weight: bfloat16 [1024, 4096], P(None, 'tensor'), may hold values from -0.1875 to 0.1875
- fc1_bias: bfloat16 [4096], P('tensor'), may hold values from -2 to 2
- fc2_weight: bfloat16 [4096, 1024], P('tensor'), may hold values from -0.1875 to 0.1875
- fc2_bias: bfloat16 [1024], replicated, may hold values from -2 to 2
Outputs:
- out: bfloat16 [21760, 1024], P('dp')
- d_tokens: bfloat16 [21760, 1024], P('dp')
- grad_table: float32 [1000, 1024], P(None, 'tensor')
- grad_ada: float32 [1024, 6144], P(None, 'tensor')
- grad_ada_bias: float32 [6144], P('tensor')
- grad_qkv: float32 [1024, 3, 1024], P(None, None, 'tensor')
- grad_q_bias: float32 [1024], P('tensor')
- grad_v_bias: float32 [1024], P('tensor')
- grad_qk_scale: float32 [16], P('tensor')
- grad_proj: float32 [1024, 1024], P('tensor')
- grad_proj_bias: float32 [1024], replicated
- grad_fc1: float32 [1024, 4096], P(None, 'tensor')
- grad_fc1_bias: float32 [4096], P('tensor')
- grad_fc2: float32 [4096, 1024], P('tensor')
- grad_fc2_bias: float32 [1024], replicated
The draws below stay inside these ranges and needn't reach their ends.
Inputs may be any that keep to these rules, and one draw needn't show every extreme that they name: `scale_ids`: in each image the scale indices never fall, each of the 10 scales holds 1 to 256 tokens, and some scale of every image holds exactly 256.
All inputs are finite; a program needn't handle non-finite values.
Results may differ from the reference program's by a relative error of at most 0.033.
Values may be sent and summed in bfloat16 or wider, within the bound.
A program may use at most 320 MiB of HBM per device.

```python
import math
import jax
import jax.numpy as jnp
import numpy as np
from jax import lax

D = 1024
HEADS = 16
FF = 4096
NCLS = 1000
SEQ = 680
SCALES = 10
LAST = 256
HEAD_DIM = 64
IMAGES = 32
TOKENS = 21760


def set_ends(array, rng, least, top_value):
    spot = [jax.random.randint(jax.random.fold_in(rng, axis), (), 0, length) for axis, length in enumerate(array.shape)]
    main_axis = array.shape.index(max(array.shape))
    neighbour = spot[:main_axis] + [(spot[main_axis] + 1) % array.shape[main_axis]] + spot[main_axis + 1:]
    return array.at[tuple(spot)].set(least).at[tuple(neighbour)].set(top_value)


def block_levels(stream_key, dims, shards, low, top_value):
    level, own = 1.0, jax.random.fold_in(stream_key, 6)
    for position, parts in shards:
        draws = jnp.exp(jax.random.uniform(jax.random.fold_in(own, position), (parts,), jnp.float32, low / len(shards), top_value / len(shards)))
        level = level * jnp.repeat(draws, dims[position] // parts).reshape([-1 if axis == position else 1 for axis in range(len(dims))])
    return level


def length_profile(amount, total, reach, lean):
    loads = [(1 << 20) // math.isqrt(rank ** lean) + 1 for rank in range(2, amount + 1)]
    spare, holding = total - reach - (amount - 1), [1] * (amount - 1)
    while spare > 0:
        movable = [i for i in range(amount - 1) if holding[i] < reach]
        pool, budget = sum([loads[i] for i in movable]), spare
        for i in movable:
            more = min(reach - holding[i], max(1, budget * loads[i] // pool), spare)
            holding[i] = holding[i] + more
            spare = spare - more
    return np.array([reach] + holding)


def uneven_parts(rng, count, total, bound, slope):
    if count == 2:
        one = jax.random.randint(rng, (), max(1, total - bound), min(bound, total - 1) + 1)
        return jnp.stack([one, total - one])
    sizes = jnp.asarray(length_profile(count, total, bound, slope), jnp.int32)
    pairs = (count - 1) // 2
    giver, taker = sizes[1:1 + 2 * pairs:2], sizes[2:2 + 2 * pairs:2]
    room = jnp.minimum(giver - 1, bound - taker)
    shifted = jax.random.randint(jax.random.fold_in(rng, 1), (pairs,), 0, 1 << 20) % (room + 1)
    sizes = sizes.at[1:1 + 2 * pairs:2].set(giver - shifted).at[2:2 + 2 * pairs:2].set(taker + shifted)
    return sizes[jax.random.permutation(jax.random.fold_in(rng, 2), count)]


def noise(own_key, shape, width, most, shards=(), held_as=jnp.bfloat16):
    gain = block_levels(own_key, shape, shards, -0.22, 0.18) if shards else 1.0
    drawn = jax.random.normal(own_key, shape, jnp.float32) * width * gain
    return jnp.minimum(jnp.maximum(drawn, -most), most).astype(held_as)


def setup_inputs(seed: int = 0) -> dict:
    splits = jax.random.split(jax.random.key(seed), 18)
    tokens = noise(splits[0], (TOKENS, D), 1.0, 6.0, ((0, 16),))
    d_out = noise(splits[1], (TOKENS, D), 1.0, 6.0, ((0, 16),))
    labels = set_ends(jax.random.randint(splits[2], (IMAGES,), 0, NCLS), jax.random.fold_in(splits[2], 1), 0, NCLS - 1).astype(jnp.int32)
    scale_ids = jax.vmap(lambda own: jnp.searchsorted(jnp.cumsum(uneven_parts(own, SCALES, SEQ, LAST, 1)), jnp.arange(SEQ), side="right"))(jax.random.split(splits[3], IMAGES)).reshape((IMAGES, SEQ)).astype(jnp.int32)
    class_table = noise(splits[4], (NCLS, D), 1.0, 6.0, ((1, 2),))
    ada_weight = noise(splits[5], (D, 6 * D), D ** -0.5, 0.1875, ((1, 2),))
    ada_bias = noise(splits[6], (6 * D,), 0.4, 3.0, ((0, 2),))
    qkv_weight = noise(splits[7], (D, 3, D), D ** -0.5, 0.1875, ((2, 2),))
    q_bias = noise(splits[8], (D,), 0.5, 3.0, ((0, 2),))
    v_bias = noise(splits[9], (D,), 0.5, 3.0, ((0, 2),))
    qk_scale = jnp.clip(2.3 + 0.70000005 * jax.random.uniform(splits[10], (HEADS,), jnp.float32) ** block_levels(splits[10], (HEADS,), ((0, 2),), -0.2, 0.2), 2.3, 3.0)
    proj_weight = noise(splits[11], (D, D), (D // 16) ** -0.5, 0.75, ((0, 2),))
    proj_bias = noise(splits[12], (D,), 0.3, 2.0)
    fc1_weight = noise(splits[13], (D, FF), D ** -0.5, 0.1875, ((1, 2),))
    fc1_bias = noise(splits[14], (FF,), 0.3, 2.0, ((0, 2),))
    fc2_weight = noise(splits[15], (FF, D), (FF // 4) ** -0.5, 0.1875, ((0, 2),))
    fc2_bias = noise(splits[16], (D,), 0.3, 2.0)
    return dict(tokens=tokens, d_out=d_out, labels=labels, scale_ids=scale_ids, class_table=class_table, ada_weight=ada_weight, ada_bias=ada_bias, qkv_weight=qkv_weight, q_bias=q_bias, v_bias=v_bias, qk_scale=qk_scale, proj_weight=proj_weight, proj_bias=proj_bias, fc1_weight=fc1_weight, fc1_bias=fc1_bias, fc2_weight=fc2_weight, fc2_bias=fc2_bias)


@jax.custom_vjp
def low(v):
    return lax.optimization_barrier(v.astype(jnp.bfloat16)).astype(jnp.float32)

@jax.custom_vjp
def low_back(v):
    return v

def low_keep(v):
    return (low(v), None)

def low_pass(kept, grad):
    return (grad,)

def back_keep(v):
    return (v, None)

def back_low(kept, grad):
    return (low(grad),)
low.defvjp(low_keep, low_pass)
low_back.defvjp(back_keep, back_low)
highest = lax.Precision.HIGHEST
epsilon = 1e-06

def layer_norm(values):
    center = values - lax.optimization_barrier(jnp.mean(values, axis=-1, keepdims=True))
    spread = lax.optimization_barrier(jnp.mean(center * center, axis=-1, keepdims=True))
    return center * lax.rsqrt(spread + epsilon)

def attend(query_low, key_low, value_low, scale_row):
    scores = low_back(jnp.einsum('she,the->hst', query_low, key_low, precision=highest))
    allowed = scale_row[None, :] <= scale_row[:, None]
    masked = jnp.where(allowed[None], scores, jnp.float32(-1e+30))
    row_max = lax.optimization_barrier(jnp.max(masked, axis=-1, keepdims=True))
    weights_exp = jnp.exp(masked - row_max)
    attn_probs = low(weights_exp / lax.optimization_barrier(jnp.sum(weights_exp, axis=-1, keepdims=True)))
    return jnp.einsum('hst,the->she', attn_probs, value_low, precision=highest)

def block(image_in, image_label, scale_row, class_table, ada_weight, ada_bias, qkv_weight, q_bias, v_bias, qk_scale, proj_weight, proj_bias, fc1_weight, fc1_bias, fc2_weight, fc2_bias):
    cond_row = class_table[image_label]
    act_cond = low(jax.nn.silu(cond_row))
    modul = low_back(jnp.dot(act_cond, ada_weight, precision=highest) + ada_bias)
    gain_one, gain_two, scale_one, scale_two, shift_one, shift_two = jnp.split(modul, 6)
    hidden_one = low(layer_norm(image_in) * (1.0 + scale_one) + shift_one)
    bias_stack = jnp.stack([q_bias, jnp.zeros_like(q_bias), v_bias])
    qkv_val = jnp.einsum('sd,dpc->spc', hidden_one, qkv_weight, precision=highest) + bias_stack[None]
    qkv_val = low_back(qkv_val).reshape(SEQ, 3, HEADS, HEAD_DIM)
    query_raw = qkv_val[:, 0]
    key_raw = qkv_val[:, 1]
    value_raw = qkv_val[:, 2]
    query_unit = query_raw * lax.rsqrt(lax.optimization_barrier(jnp.sum(query_raw * query_raw, axis=-1, keepdims=True)) + epsilon)
    key_unit = key_raw * lax.rsqrt(lax.optimization_barrier(jnp.sum(key_raw * key_raw, axis=-1, keepdims=True)) + epsilon)
    query_low = low(query_unit * jnp.exp(qk_scale)[None, :, None])
    attn_raw = jax.checkpoint(attend)(query_low, low(key_unit), low(value_raw), scale_row)
    attn_out = low_back(low(attn_raw.reshape(SEQ, D)))
    branch_one = low_back(jnp.dot(attn_out, proj_weight, precision=highest) + proj_bias)
    middle = image_in + gain_one * branch_one
    hidden_two = low(layer_norm(middle) * (1.0 + scale_two) + shift_two)
    pre_act = low_back(jnp.dot(hidden_two, fc1_weight, precision=highest) + fc1_bias)
    mlp_act = low(jax.nn.gelu(pre_act, approximate=True))
    branch_two = low_back(jnp.dot(mlp_act, fc2_weight, precision=highest) + fc2_bias)
    return middle + gain_two * branch_two

def reference(tokens, d_out, labels, scale_ids, class_table, ada_weight, ada_bias, qkv_weight, q_bias, v_bias, qk_scale, proj_weight, proj_bias, fc1_weight, fc1_bias, fc2_weight, fc2_bias):
    params = tuple((item.astype(jnp.float32) for item in (class_table, ada_weight, ada_bias, qkv_weight, q_bias, v_bias, qk_scale, proj_weight, proj_bias, fc1_weight, fc1_bias, fc2_weight, fc2_bias)))
    token_images = tokens.astype(jnp.float32).reshape(IMAGES, SEQ, D)
    cot_images = d_out.astype(jnp.float32).reshape(IMAGES, SEQ, D)

    def one_image(running, inputs):
        image_in, image_cot, image_label, scale_row = inputs

        def inner(source, *weights):
            return block(source, image_label, scale_row, *weights)
        block_out, pullback = jax.vjp(inner, image_in, *params)
        grads = pullback(image_cot)
        running = tuple((acc + new for acc, new in zip(running, grads[1:])))
        return (running, (block_out, grads[0]))
    start = tuple((jnp.zeros_like(item) for item in params))
    sums, (outputs, input_grads) = lax.scan(one_image, start, (token_images, cot_images, labels.astype(jnp.int32), scale_ids.astype(jnp.int32)))
    return (outputs.reshape(TOKENS, D).astype(jnp.bfloat16), input_grads.reshape(TOKENS, D).astype(jnp.bfloat16), sums[0], sums[1], sums[2], sums[3], sums[4], sums[5], sums[6], sums[7], sums[8], sums[9], sums[10], sums[11], sums[12])
```

```python
from functools import partial

import jax
import jax.numpy as jnp
from jax import lax
from jax.sharding import PartitionSpec as P

epsilon = 1e-06
highest = lax.Precision.HIGHEST


def tensor_sum(part):
    if lax.axis_size("tensor") == 2:
        other = lax.ppermute(part, "tensor", [(0, 1), (1, 0)])
        return part.astype(jnp.float32) + other.astype(jnp.float32)
    return lax.psum(part, "tensor").astype(jnp.float32)


def layer_stats(values):
    center = values - jnp.mean(values, axis=-1, keepdims=True)
    inv_std = lax.rsqrt(jnp.mean(center * center, axis=-1, keepdims=True) + epsilon)
    return (center * inv_std, inv_std)


def layer_back(d_normed, normed, inv_std):
    first_mean = jnp.mean(d_normed, axis=-1, keepdims=True)
    second_mean = jnp.mean(d_normed * normed, axis=-1, keepdims=True)
    return inv_std * (d_normed - first_mean - normed * second_mean)


def per_device(
    tokens,
    d_out,
    labels,
    scale_ids,
    class_table,
    ada_weight,
    ada_bias,
    qkv_weight,
    q_bias,
    v_bias,
    qk_scale,
    proj_weight,
    proj_bias,
    fc1_weight,
    fc1_bias,
    fc2_weight,
    fc2_bias,
):
    f32 = jnp.float32
    bf16 = jnp.bfloat16
    images = scale_ids.shape[0]
    length = scale_ids.shape[1]
    model_width = tokens.shape[1]
    rows_all = images * length
    classes = class_table.shape[0]
    heads_here = qk_scale.shape[0]
    local_width = qkv_weight.shape[2]
    head_size = local_width // heads_here
    mod_width = ada_weight.shape[1]
    first_image = lax.axis_index("dp") * images
    class_ids = jnp.arange(classes, dtype=jnp.int32)
    pick_all = labels[:, None] == class_ids[None, :]
    cond_all_cols = jnp.dot(pick_all.astype(bf16), class_table, preferred_element_type=f32)
    cond_all = lax.all_gather(cond_all_cols.astype(bf16), "tensor", axis=1, tiled=True)
    cond_full = lax.dynamic_slice_in_dim(cond_all, first_image, images)
    act_cond = jax.nn.silu(cond_full.astype(f32)).astype(bf16)
    mod_cols = jnp.dot(act_cond, ada_weight, preferred_element_type=f32) + ada_bias.astype(f32)
    modul = lax.all_gather(mod_cols, "tensor", axis=1, tiled=True)
    gain_one, gain_two, scale_one, scale_two, shift_one, shift_two = [
        modul[:, None, member * model_width : (member + 1) * model_width] for member in range(6)
    ]
    inputs = tokens.astype(f32).reshape(images, length, model_width)
    normed_one, inv_std_one = layer_stats(inputs)
    hidden_one = (
        (normed_one * (1.0 + scale_one) + shift_one).astype(bf16).reshape(rows_all, model_width)
    )
    bias_stack = jnp.stack([q_bias.astype(f32), jnp.zeros(q_bias.shape, f32), v_bias.astype(f32)])
    qkv_val = (
        jnp.einsum("rd,dpc->rpc", hidden_one, qkv_weight, preferred_element_type=f32)
        + bias_stack[None]
    )
    qkv_val = qkv_val.reshape(images, length, 3, heads_here, head_size)
    query_raw = qkv_val[:, :, 0]
    key_raw = qkv_val[:, :, 1]
    value_raw = qkv_val[:, :, 2]
    query_inv = lax.rsqrt(jnp.sum(query_raw * query_raw, axis=-1, keepdims=True) + epsilon)
    query_unit = query_raw * query_inv
    growth = jnp.exp(qk_scale)[None, None, :, None]
    query_scaled = query_unit * growth
    query_low = query_scaled.astype(bf16)
    key_inv = lax.rsqrt(jnp.sum(key_raw * key_raw, axis=-1, keepdims=True) + epsilon)
    key_unit = key_raw * key_inv
    key_low = key_unit.astype(bf16)
    value_low = value_raw.astype(bf16)
    allowed = scale_ids[:, None, None, :] <= scale_ids[:, None, :, None]

    def masked_scores():
        scores = jnp.einsum("ishe,ithe->ihst", query_low, key_low, preferred_element_type=f32)
        return jnp.where(allowed, scores, f32(-1e30))

    masked = masked_scores()
    row_max = jnp.max(masked, axis=-1, keepdims=True)
    weights_exp = jnp.exp(masked - row_max)
    row_total = jnp.sum(weights_exp, axis=-1, keepdims=True)
    log_total = row_max + jnp.log(row_total)
    probs_low = (weights_exp / row_total).astype(bf16)
    attn_out = (
        jnp.einsum("ihst,ithe->ishe", probs_low, value_low, preferred_element_type=f32)
        .reshape(rows_all, local_width)
        .astype(bf16)
    )
    gelu_tanh = partial(jax.nn.gelu, approximate=True)
    d_result = d_out.astype(f32).reshape(images, length, model_width)
    branch_one = tensor_sum(jnp.dot(attn_out, proj_weight, preferred_element_type=f32).astype(bf16))
    branch_one = (branch_one + proj_bias.astype(f32)).reshape(images, length, model_width)
    middle = inputs + gain_one * branch_one
    normed_two, inv_std_two = layer_stats(middle)
    hidden_two = (
        (normed_two * (1.0 + scale_two) + shift_two).astype(bf16).reshape(rows_all, model_width)
    )
    pre_act = jnp.dot(hidden_two, fc1_weight, preferred_element_type=f32) + fc1_bias.astype(f32)
    mlp_low = gelu_tanh(pre_act).astype(bf16)
    branch_two = tensor_sum(jnp.dot(mlp_low, fc2_weight, preferred_element_type=f32).astype(bf16))
    branch_two = (branch_two + fc2_bias.astype(f32)).reshape(images, length, model_width)
    result = (middle + gain_two * branch_two).astype(bf16).reshape(rows_all, model_width)
    d_branch_two = (gain_two * d_result).astype(bf16).reshape(rows_all, model_width)
    grad_fc2 = jnp.einsum("rf,rd->fd", mlp_low, d_branch_two, preferred_element_type=f32)
    grad_fc2_bias = jnp.sum(d_branch_two.astype(f32), axis=0)
    d_mlp = jnp.einsum("rd,fd->rf", d_branch_two, fc2_weight, preferred_element_type=f32)
    gelu_value, gelu_pull = jax.vjp(gelu_tanh, pre_act)
    d_pre = gelu_pull(d_mlp)[0].astype(bf16)
    grad_fc1 = jnp.einsum("rd,rf->df", hidden_two, d_pre, preferred_element_type=f32)
    grad_fc1_bias = jnp.sum(d_pre.astype(f32), axis=0)
    d_hidden_two = tensor_sum(
        jnp.einsum("rf,df->rd", d_pre, fc1_weight, preferred_element_type=f32).astype(bf16)
    )
    d_hidden_two = d_hidden_two.reshape(images, length, model_width)
    d_middle = d_result + layer_back(d_hidden_two * (1.0 + scale_two), normed_two, inv_std_two)
    d_branch_one = (gain_one * d_middle).astype(bf16).reshape(rows_all, model_width)
    grad_proj = jnp.einsum("rc,rd->cd", attn_out, d_branch_one, preferred_element_type=f32)
    grad_proj_bias = jnp.sum(d_branch_one.astype(f32), axis=0)
    d_attn = jnp.einsum("rd,cd->rc", d_branch_one, proj_weight, preferred_element_type=f32).astype(
        bf16
    )
    d_attn = d_attn.reshape(images, length, heads_here, head_size)
    again_probs = jnp.exp(masked_scores() - log_total)
    again_low = again_probs.astype(bf16)
    d_probs = jnp.einsum("ishe,ithe->ihst", d_attn, value_low, preferred_element_type=f32)
    d_scores = (
        again_probs * (d_probs - jnp.sum(again_probs * d_probs, axis=-1, keepdims=True))
    ).astype(bf16)
    d_query_scaled = jnp.einsum("ihst,ithe->ishe", d_scores, key_low, preferred_element_type=f32)
    d_key_unit = jnp.einsum("ihst,ishe->ithe", d_scores, query_low, preferred_element_type=f32)
    d_value = jnp.einsum("ihst,ishe->ithe", again_low, d_attn, preferred_element_type=f32)
    grad_scale = jnp.sum(d_query_scaled * query_scaled, axis=(0, 1, 3))
    d_query_unit = d_query_scaled * growth
    d_query = query_inv * (
        d_query_unit - query_unit * jnp.sum(d_query_unit * query_unit, axis=-1, keepdims=True)
    )
    d_key = key_inv * (
        d_key_unit - key_unit * jnp.sum(d_key_unit * key_unit, axis=-1, keepdims=True)
    )
    d_qkv = (
        jnp.stack([d_query, d_key, d_value], axis=2).reshape(rows_all, 3, local_width).astype(bf16)
    )
    grad_q_bias = jnp.sum(d_qkv[:, 0].astype(f32), axis=0)
    grad_v_bias = jnp.sum(d_qkv[:, 2].astype(f32), axis=0)
    grad_qkv = jnp.einsum("rd,rpc->dpc", hidden_one, d_qkv, preferred_element_type=f32)
    d_hidden_one = tensor_sum(
        jnp.einsum("rpc,dpc->rd", d_qkv, qkv_weight, preferred_element_type=f32).astype(bf16)
    )
    d_hidden_one = d_hidden_one.reshape(images, length, model_width)
    d_inputs = d_middle + layer_back(d_hidden_one * (1.0 + scale_one), normed_one, inv_std_one)
    d_tokens = d_inputs.astype(bf16).reshape(rows_all, model_width)
    d_modul = jnp.concatenate(
        [
            jnp.sum(d_middle * branch_one, axis=1),
            jnp.sum(d_result * branch_two, axis=1),
            jnp.sum(d_hidden_one * normed_one, axis=1),
            jnp.sum(d_hidden_two * normed_two, axis=1),
            jnp.sum(d_hidden_one, axis=1),
            jnp.sum(d_hidden_two, axis=1),
        ],
        axis=1,
    ).astype(bf16)
    col_start = lax.axis_index("tensor") * mod_width
    dmod_cols = lax.dynamic_slice_in_dim(d_modul, col_start, mod_width, 1)
    dmod_all = lax.all_gather(dmod_cols, "dp", axis=0, tiled=True)
    small = [grad_q_bias, grad_v_bias, grad_scale, grad_proj_bias, grad_fc1_bias, grad_fc2_bias]
    sizes = [item.shape[0] for item in small]
    packed = lax.all_gather(jnp.concatenate(small), "dp", axis=0, tiled=False)
    packed = jnp.sum(packed, axis=0)
    ends = [sum(sizes[: k + 1]) for k in range(len(sizes))]
    grad_q_bias, grad_v_bias, grad_scale, grad_proj_bias, grad_fc1_bias, grad_fc2_bias = [
        packed[e - n : e] for e, n in zip(ends, sizes)
    ]
    act_all = jax.nn.silu(cond_all.astype(f32)).astype(bf16)
    d_act_part = jnp.einsum("ic,dc->id", dmod_all, ada_weight, preferred_element_type=f32)
    d_act_cols = lax.psum_scatter(d_act_part, "tensor", scatter_dimension=1, tiled=True)
    silu_value, silu_pull = jax.vjp(jax.nn.silu, cond_all_cols)
    d_cond = silu_pull(d_act_cols)[0]
    grad_table = jnp.einsum(
        "in,ic->nc", pick_all.astype(f32), d_cond, precision=highest, preferred_element_type=f32
    )
    grad_ada = jnp.einsum("id,ic->dc", act_all, dmod_all, preferred_element_type=f32)
    grad_ada_bias = jnp.sum(dmod_all.astype(f32), axis=0)
    grad_qkv, grad_proj, grad_fc1, grad_fc2 = (
        lax.psum(grad_qkv.astype(bf16), "dp").astype(f32),
        lax.psum(grad_proj.astype(bf16), "dp").astype(f32),
        lax.psum(grad_fc1.astype(bf16), "dp").astype(f32),
        lax.psum(grad_fc2.astype(bf16), "dp").astype(f32),
    )
    return (
        result,
        d_tokens,
        grad_table,
        grad_ada,
        grad_ada_bias,
        grad_qkv,
        grad_q_bias,
        grad_v_bias,
        grad_scale,
        grad_proj,
        grad_proj_bias,
        grad_fc1,
        grad_fc1_bias,
        grad_fc2,
        grad_fc2_bias,
    )


def solution(mesh):
    return jax.shard_map(
        per_device,
        mesh=mesh,
        in_specs=(
            P("dp", None),
            P("dp", None),
            P(),
            P("dp", None),
            P(None, "tensor"),
            P(None, "tensor"),
            P("tensor"),
            P(None, None, "tensor"),
            P("tensor"),
            P("tensor"),
            P("tensor"),
            P("tensor", None),
            P(),
            P(None, "tensor"),
            P("tensor"),
            P("tensor", None),
            P(),
        ),
        out_specs=(
            P("dp", None),
            P("dp", None),
            P(None, "tensor"),
            P(None, "tensor"),
            P("tensor"),
            P(None, None, "tensor"),
            P("tensor"),
            P("tensor"),
            P("tensor"),
            P("tensor", None),
            P(),
            P(None, "tensor"),
            P("tensor"),
            P("tensor", None),
            P(),
        ),
        check_vma=False,
    )
```

```python
from functools import partial

import jax
import jax.numpy as jnp
from jax import lax
from jax.experimental import pallas as pl
from jax.experimental.pallas import tpu as pltpu
from jax.sharding import PartitionSpec as P

epsilon = 1e-06
highest = lax.Precision.HIGHEST
CHUNKS = 4

def padded(length):
    return -(-length // 256) * 256, -(-length // (16 * CHUNKS)) * 16

def head_sums(values, low_half):
    first = jnp.sum(jnp.where(low_half, values, 0.0), axis=-1, keepdims=True)
    second = jnp.sum(jnp.where(low_half, 0.0, values), axis=-1, keepdims=True)
    return first, second

def unit_heads(raw, low_half):
    first, second = head_sums(raw * raw, low_half)
    inv = jnp.where(low_half, lax.rsqrt(first + epsilon), lax.rsqrt(second + epsilon))
    return raw * inv, inv

def lane_facts(length):
    lane = lax.broadcasted_iota(jnp.int32, (length, 128), 1)
    return lane < 64, lane & 63

def fill(ref, value):
    rows = value.shape[0]
    ref[:rows, :] = value.astype(ref.dtype)
    ref[rows:, :] = jnp.zeros((ref.shape[0] - rows, ref.shape[1]), ref.dtype)

def fwd_kernel(qkv_ref, sid_ref, growth_ref, out_ref, q_s, k_s, v_s):
    f32, bf16 = jnp.float32, jnp.bfloat16
    length = out_ref.shape[0]
    cols, step = padded(length)
    low_half, slot = lane_facts(length)
    sid = sid_ref[0]
    query, _ = unit_heads(qkv_ref[0, 0], low_half)
    key, _ = unit_heads(qkv_ref[1, 0], low_half)
    query = query * growth_ref[...]
    value = qkv_ref[2, 0]
    hide = jnp.where((slot > sid) & (slot < 16), -1e30, 0.0)
    own = jnp.where(slot == sid, 1.0, 0.0)
    for head in range(2):
        mine = low_half if head == 0 else ~low_half
        fill(q_s.at[head], jnp.where(mine, query, hide))
        fill(k_s.at[head], jnp.where(mine, key, own))
        fill(v_s.at[head], jnp.where(mine, value, 1.0))
    for chunk in range(CHUNKS):
        first = chunk * step
        rows = min(step, length - first)
        parts = []
        for head in range(2):
            scores = lax.dot_general(q_s[head, first : first + step, :], k_s[head], (((1,), (1,)), ((), ())), preferred_element_type=f32)
            weights = jnp.exp(scores).astype(bf16)
            parts.append(jnp.dot(weights, v_s[head], preferred_element_type=f32))
        half = low_half[:1]
        total = jnp.where(half, parts[1], parts[0])
        mixed = jnp.where(half, parts[0], parts[1]) / pltpu.roll(total, 64, 1)
        out_ref[first : first + rows, :] = mixed[:rows].astype(bf16)

def bwd_kernel(qkv_ref, sid_ref, growth_ref, dout_ref, dqkv_ref, sums_ref,
               q_s, k_s, v_s, do_s, qp_s, kp_s, dop_s, dst_s, weight_s, product_s):
    f32, bf16 = jnp.float32, jnp.bfloat16
    length = dout_ref.shape[0]
    cols, step = padded(length)
    low_half, slot = lane_facts(length)
    sid = sid_ref[0]
    query_unit, query_inv = unit_heads(qkv_ref[0, 0], low_half)
    key_unit, key_inv = unit_heads(qkv_ref[1, 0], low_half)
    query = query_unit * growth_ref[...]
    value = qkv_ref[2, 0]
    dout = dout_ref[...].astype(f32)
    hide = jnp.where((slot > sid) & (slot < 16), -1e30, 0.0)
    own = jnp.where(slot == sid, 1.0, 0.0)
    fill(qp_s, query)
    fill(kp_s, key_unit)
    fill(dop_s, dout)
    fill(v_s, value)
    for head in range(2):
        mine = low_half if head == 0 else ~low_half
        fill(q_s.at[head], jnp.where(mine, query, hide))
        fill(k_s.at[head], jnp.where(mine, key_unit, own))
        fill(do_s.at[head], jnp.where(mine, dout, 0.0))
    half = low_half[:1]
    d_key, d_value, d_query = [], [], []
    nt = (((1,), (1,)), ((), ()))
    for head in range(2):
        dks, dvs = [], []
        total, inner = jnp.zeros((1, cols), f32), jnp.zeros((1, cols), f32)
        for chunk in range(CHUNKS):
            rows = slice(chunk * step, (chunk + 1) * step)
            scores = lax.dot_general(k_s[head, rows, :], q_s[head], nt, preferred_element_type=f32)
            weights = jnp.exp(scores)
            if (chunk + 1) * step > length:
                row = lax.broadcasted_iota(jnp.int32, (step, cols), 0)
                weights = jnp.where(row < length - chunk * step, weights, 0.0)
            d_probs = lax.dot_general(v_s[rows, :], do_s[head], nt, preferred_element_type=f32)
            product = weights * d_probs
            weight_s[rows, :] = weights
            product_s[rows, :] = product
            total = total + jnp.sum(weights, axis=0, keepdims=True)
            inner = inner + jnp.sum(product, axis=0, keepdims=True)
        inv = 1.0 / total
        inner = inner * inv
        for chunk in range(CHUNKS):
            rows = slice(chunk * step, (chunk + 1) * step)
            probs = weight_s[rows, :] * inv
            d_scores = (product_s[rows, :] * inv - probs * inner).astype(bf16)
            dst_s[rows, :] = d_scores
            dvs.append(jnp.dot(probs.astype(bf16), dop_s[...], preferred_element_type=f32))
            dks.append(jnp.dot(d_scores, qp_s[...], preferred_element_type=f32))
        if CHUNKS * step < cols:
            dst_s[CHUNKS * step :, :] = jnp.zeros((cols - CHUNKS * step, cols), bf16)
        d_query.append(lax.dot_general(dst_s[...], kp_s[...], (((0,), (0,)), ((), ())), preferred_element_type=f32))
        d_key.append(jnp.concatenate(dks, axis=0))
        d_value.append(jnp.concatenate(dvs, axis=0))
    pick = lambda pair: jnp.where(half, pair[0], pair[1])[:length]
    d_query, d_key, d_value = pick(d_query), pick(d_key), pick(d_value)
    sums_ref[0:1, :] = jnp.sum(d_query * query, axis=0, keepdims=True)

    def back(d_unit, unit, inv):
        first, second = head_sums(d_unit * unit, low_half)
        return inv * (d_unit - unit * jnp.where(low_half, first, second))

    d_query = back(d_query * growth_ref[...], query_unit, query_inv).astype(bf16)
    d_key = back(d_key, key_unit, key_inv).astype(bf16)
    d_value = d_value.astype(bf16)
    dqkv_ref[0] = d_query
    dqkv_ref[1] = d_key
    dqkv_ref[2] = d_value
    sums_ref[1:2, :] = jnp.sum(d_query.astype(f32), axis=0, keepdims=True)
    sums_ref[2:3, :] = jnp.sum(d_value.astype(f32), axis=0, keepdims=True)
    sums_ref[3:8, :] = jnp.zeros((5, 128), f32)


def attention(qkv, sid, growth, image):
    _, _, length, width = qkv.shape
    cols, _ = padded(length)
    n = width // 64 * length * length
    return pl.pallas_call(
        fwd_kernel,
        grid=(width // 128,),
        in_specs=[
            pl.BlockSpec((3, 1, length, 128), lambda h: (0, image, 0, h)),
            pl.BlockSpec((1, length, 1), lambda h: (image, 0, 0)),
            pl.BlockSpec((1, 128), lambda h: (0, h)),
        ],
        out_specs=pl.BlockSpec((length, 128), lambda h: (0, h)),
        out_shape=jax.ShapeDtypeStruct((length, width), jnp.bfloat16),
        scratch_shapes=[pltpu.VMEM((2, cols, 128), jnp.bfloat16)] * 3,
        cost_estimate=pl.CostEstimate(flops=16 * 64 * n, transcendentals=n, bytes_accessed=14 * length * width),
        compiler_params=pltpu.CompilerParams(vmem_limit_bytes=48 << 20),
        name="attend",
    )(qkv, sid, growth)


def attention_back(qkv, sid, growth, dout, image):
    _, _, length, width = qkv.shape
    cols, step = padded(length)
    n = width // 64 * length * length
    two = pltpu.VMEM((2, cols, 128), jnp.bfloat16)
    one = pltpu.VMEM((cols, 128), jnp.bfloat16)
    wide = pltpu.VMEM((CHUNKS * step, cols), jnp.float32)
    return pl.pallas_call(
        bwd_kernel,
        grid=(width // 128,),
        in_specs=[
            pl.BlockSpec((3, 1, length, 128), lambda h: (0, image, 0, h)),
            pl.BlockSpec((1, length, 1), lambda h: (image, 0, 0)),
            pl.BlockSpec((1, 128), lambda h: (0, h)),
            pl.BlockSpec((length, 128), lambda h: (0, h)),
        ],
        out_specs=[pl.BlockSpec((3, length, 128), lambda h: (0, 0, h)), pl.BlockSpec((8, 128), lambda h: (0, h))],
        out_shape=[
            jax.ShapeDtypeStruct((3, length, width), jnp.bfloat16),
            jax.ShapeDtypeStruct((8, width), jnp.float32),
        ],
        scratch_shapes=[two, two, one, two, one, one, one, pltpu.VMEM((cols, cols), jnp.bfloat16), wide, wide],
        cost_estimate=pl.CostEstimate(flops=40 * 64 * n, transcendentals=n, bytes_accessed=20 * length * width),
        compiler_params=pltpu.CompilerParams(vmem_limit_bytes=56 << 20),
        name="attend_back",
    )(qkv, sid, growth, dout)


def after(value, *others):
    return lax.optimization_barrier((value, *others))[0]


def tensor_pair():
    return lax.axis_size("tensor") == 2


def tensor_swap(part):
    return lax.ppermute(part, "tensor", [(0, 1), (1, 0)])


def tensor_sum(part, *late):
    if tensor_pair():
        other = tensor_swap(part)
        if late:
            other = after(other, *late)
        return part.astype(jnp.float32) + other.astype(jnp.float32)
    return lax.psum(part, "tensor").astype(jnp.float32)


def joined(part, other, first, axis):
    return jnp.concatenate([jnp.where(first, part, other), jnp.where(first, other, part)], axis=axis)


def tensor_gather(part, axis):
    if tensor_pair():
        return joined(part, tensor_swap(part), lax.axis_index("tensor") == 0, axis)
    return lax.all_gather(part, "tensor", axis=axis, tiled=True)


def tensor_scatter(part):
    if tensor_pair():
        half = part.shape[1] // 2
        me = lax.axis_index("tensor")
        mine = lax.dynamic_slice_in_dim(part, me * half, half, 1)
        return mine + tensor_swap(lax.dynamic_slice_in_dim(part, (1 - me) * half, half, 1))
    return lax.psum_scatter(part, "tensor", scatter_dimension=1, tiled=True)


def grad_sum(make, shape, axis, pieces=1):
    bf16, f32 = jnp.bfloat16, jnp.float32
    rows = shape[axis]
    if lax.axis_size("dp") != 16:
        return lax.psum(make(0, rows).astype(bf16), "dp").astype(f32)
    index = lax.axis_index("dp")
    low, high, line = index % 2, index // 2 % 2, index // 4
    half, quarter = rows // 2, rows // 4
    cut = partial(lax.dynamic_slice_in_dim, axis=axis)
    swap = lambda value, bit: lax.ppermute(value, "dp", [(i, i ^ bit) for i in range(16)])

    def hop(value, moves):
        return lax.ppermute(value, "dp", [(4 * a + k, 4 * b + k) for a, b in moves for k in range(4)])

    theirs = make((1 - low) * half, half).astype(bf16)
    got = swap(theirs, 1)
    mine = make(low * half, half).astype(bf16)
    add = lambda first: (cut(mine, first, quarter).astype(f32) + cut(got, first, quarter).astype(f32)).astype(bf16)
    got_high = swap(add((1 - high) * quarter), 2)
    part = (add(high * quarter).astype(f32) + got_high.astype(f32)).astype(bf16)
    inner = (line == 1) | (line == 2)
    sums = []
    for piece in jnp.split(part, pieces, axis=axis):
        piece = (piece.astype(f32) + hop(piece, [(0, 1), (3, 2)]).astype(f32)).astype(bf16)
        piece = (piece.astype(f32) + hop(piece, [(1, 2), (2, 1)]).astype(f32)).astype(bf16)
        sums.append(jnp.where(inner, piece, hop(piece, [(1, 0), (2, 3)])))
    total = jnp.concatenate(sums, axis=axis) if pieces > 1 else sums[0]
    total = joined(total, swap(total, 2), high == 0, axis)
    return joined(total, swap(total, 1), low == 0, axis).astype(f32)


def layer_stats(values):
    center = values - jnp.mean(values, axis=-1, keepdims=True)
    inv_std = lax.rsqrt(jnp.mean(center * center, axis=-1, keepdims=True) + epsilon)
    return (center * inv_std, inv_std)


def layer_back(d_normed, normed, inv_std):
    first_mean = jnp.mean(d_normed, axis=-1, keepdims=True)
    second_mean = jnp.mean(d_normed * normed, axis=-1, keepdims=True)
    return inv_std * (d_normed - first_mean - normed * second_mean)


def per_device(
    tokens,
    d_out,
    labels,
    scale_ids,
    class_table,
    ada_weight,
    ada_bias,
    qkv_weight,
    q_bias,
    v_bias,
    qk_scale,
    proj_weight,
    proj_bias,
    fc1_weight,
    fc1_bias,
    fc2_weight,
    fc2_bias,
):
    f32 = jnp.float32
    bf16 = jnp.bfloat16
    dot = partial(jnp.dot, preferred_element_type=f32)
    ein = partial(jnp.einsum, preferred_element_type=f32)
    images, length = scale_ids.shape
    width = tokens.shape[1]
    classes = class_table.shape[0]
    heads_here = qk_scale.shape[0]
    local_width = qkv_weight.shape[2]
    head_size = local_width // heads_here
    mod_width = ada_weight.shape[1]
    every = range(images)
    rows = [slice(i * length, (i + 1) * length) for i in every]
    first_image = lax.axis_index("dp") * images

    class_ids = jnp.arange(classes, dtype=jnp.int32)
    pick_all = labels[:, None] == class_ids[None, :]
    cond_cols = dot(pick_all.astype(bf16), class_table)
    cond_all = tensor_gather(cond_cols.astype(bf16), 1)
    act_all = jax.nn.silu(cond_all.astype(f32)).astype(bf16)
    act_mine = lax.dynamic_slice_in_dim(act_all, first_image, images)
    mod_cols = dot(act_mine, ada_weight) + ada_bias.astype(f32)
    modul = tensor_gather(mod_cols, 1)
    proj_full = tensor_gather(after(proj_weight, modul), 0)
    gain_one, gain_two, scale_one, scale_two, shift_one, shift_two = [
        [modul[i : i + 1, member * width : (member + 1) * width] for i in every] for member in range(6)
    ]
    inputs = [tokens[rows[i]].astype(f32) for i in every]
    d_result = [d_out[rows[i]].astype(f32) for i in every]

    sid = scale_ids[:, :, None]
    growth = jnp.repeat(jnp.exp(qk_scale), head_size)[None]
    normed_one, inv_one = zip(*[layer_stats(inputs[i]) for i in every])
    hidden_one = jnp.concatenate(
        [(normed_one[i] * (1.0 + scale_one[i]) + shift_one[i]).astype(bf16) for i in every], axis=0
    )
    bias_stack = jnp.stack([q_bias.astype(f32), jnp.zeros(q_bias.shape, f32), v_bias.astype(f32)])
    qkv = ein("rd,dpc->prc", hidden_one, qkv_weight) + bias_stack[:, None, :]
    qkv = qkv.reshape(3, images, length, local_width)

    gelu_tanh = partial(jax.nn.gelu, approximate=True)
    attn, branch_one, middle, normed_two, inv_two = [], [], [], [], []
    hidden_two, pre_act, d_pre, d_hidden_two, parts = [], [], [], [], []
    d_branch_two = jnp.concatenate([(gain_two[i] * d_result[i]).astype(bf16) for i in every], axis=0)
    for i in every:
        attn.append(attention(qkv, sid, growth, i))
    for i in every:
        branch_one.append(dot(tensor_gather(attn[i], 1), proj_full) + proj_bias.astype(f32))
        middle.append(inputs[i] + gain_one[i] * branch_one[i])
        normed, inv = layer_stats(middle[i])
        normed_two.append(normed)
        inv_two.append(inv)
        hidden_two.append((normed * (1.0 + scale_two[i]) + shift_two[i]).astype(bf16))
        pre_act.append(dot(hidden_two[i], fc1_weight) + fc1_bias.astype(f32))
        d_mlp = ein("rd,fd->rf", d_branch_two[rows[i]], fc2_weight)
        gelu_value, gelu_pull = jax.vjp(gelu_tanh, pre_act[i])
        d_pre.append(gelu_pull(d_mlp)[0].astype(bf16))
        parts.append(ein("rf,df->rd", d_pre[i], fc1_weight).astype(bf16))
        d_hidden_two.append(tensor_sum(parts[i]))
    mlp_low = jnp.concatenate([gelu_tanh(pre_act[i]).astype(bf16) for i in every], axis=0)
    mlp_low = after(mlp_low, parts[-1])
    hidden_two = after(jnp.concatenate(hidden_two, axis=0), parts[-1])
    d_pre_all = after(jnp.concatenate(d_pre, axis=0), parts[-1])
    cols = partial(lax.dynamic_slice_in_dim, axis=1)
    grad_fc2 = grad_sum(lambda a, n: ein("rf,rd->fd", cols(mlp_low, a, n), d_branch_two), fc2_weight.shape, 0)
    grad_fc1 = grad_sum(lambda a, n: ein("rd,rf->df", cols(hidden_two, a, n), d_pre_all), fc1_weight.shape, 0)
    grad_fc2_bias = jnp.sum(d_branch_two.astype(f32), axis=0)
    grad_fc1_bias = jnp.sum(d_pre_all.astype(f32), axis=0)
    parts_two = [dot(mlp_low[rows[i]], fc2_weight).astype(bf16) for i in every]
    d_middle, d_branch_one, d_qkv, sums, d_hidden_one = [], [], [], [], []
    for i in every:
        d_middle.append(
            d_result[i] + layer_back(d_hidden_two[i] * (1.0 + scale_two[i]), normed_two[i], inv_two[i])
        )
        d_branch_one.append((gain_one[i] * d_middle[i]).astype(bf16))
        d_attn = ein("rd,cd->rc", d_branch_one[i], proj_weight).astype(bf16)
        d_qkv_i, sums_i = attention_back(qkv, sid, growth, d_attn, i)
        d_qkv.append(d_qkv_i)
        sums.append(sums_i)
        d_hidden_one.append(tensor_sum(ein("prc,dpc->rd", d_qkv_i, qkv_weight).astype(bf16)))
    branch_two = [tensor_sum(parts_two[i], d_qkv[-1]) + fc2_bias.astype(f32) for i in every]
    d_branch_one = jnp.concatenate(d_branch_one, axis=0)
    attn = jnp.concatenate(attn, axis=0)
    grad_proj = grad_sum(lambda a, n: ein("rc,rd->cd", cols(attn, a, n), d_branch_one), proj_weight.shape, 0)
    grad_proj_bias = jnp.sum(d_branch_one.astype(f32), axis=0)
    d_qkv = jnp.concatenate(d_qkv, axis=1)
    grad_qkv = grad_sum(
        lambda a, n: ein("rd,prc->pdc", cols(hidden_one, a, n), d_qkv), (3, width, local_width), 1, 2
    )
    grad_qkv = jnp.transpose(grad_qkv, (1, 0, 2))
    sums = sum(sums)
    grad_scale = jnp.sum(sums[0].reshape(heads_here, head_size), axis=1)
    grad_q_bias, grad_v_bias = sums[1], sums[2]
    result = jnp.concatenate(
        [(middle[i] + gain_two[i] * branch_two[i]).astype(bf16) for i in every], axis=0
    )
    d_tokens, d_modul = [], []
    for i in every:
        back = layer_back(d_hidden_one[i] * (1.0 + scale_one[i]), normed_one[i], inv_one[i])
        d_tokens.append((d_middle[i] + back).astype(bf16))
        d_modul.append(
            jnp.concatenate(
                [
                    jnp.sum(d_middle[i] * branch_one[i], axis=0),
                    jnp.sum(d_result[i] * branch_two[i], axis=0),
                    jnp.sum(d_hidden_one[i] * normed_one[i], axis=0),
                    jnp.sum(d_hidden_two[i] * normed_two[i], axis=0),
                    jnp.sum(d_hidden_one[i], axis=0),
                    jnp.sum(d_hidden_two[i], axis=0),
                ]
            ).astype(bf16)
        )
    d_tokens = jnp.concatenate(d_tokens, axis=0)
    col_start = lax.axis_index("tensor") * mod_width
    dmod_cols = lax.dynamic_slice_in_dim(jnp.stack(d_modul), col_start, mod_width, 1)
    dmod_all = lax.all_gather(dmod_cols, "dp", axis=0, tiled=True)
    small = [grad_q_bias, grad_v_bias, grad_scale, grad_proj_bias, grad_fc1_bias, grad_fc2_bias]
    sizes = [item.shape[0] for item in small]
    padding = -sum(sizes) % 1024
    packed = jnp.concatenate([*small, jnp.zeros((padding,), f32)]).reshape(1, -1, 128)
    packed = jnp.sum(lax.all_gather(packed, "dp", axis=0, tiled=True), axis=0).reshape(-1)
    ends = [sum(sizes[: k + 1]) for k in range(len(sizes))]
    grad_q_bias, grad_v_bias, grad_scale, grad_proj_bias, grad_fc1_bias, grad_fc2_bias = [
        packed[e - n : e] for e, n in zip(ends, sizes)
    ]
    d_act_part = ein("ic,dc->id", dmod_all, ada_weight)
    d_act_cols = tensor_scatter(d_act_part)
    silu_value, silu_pull = jax.vjp(jax.nn.silu, cond_cols)
    d_cond = silu_pull(d_act_cols)[0]
    grad_table = ein("in,ic->nc", pick_all.astype(f32), d_cond, precision=highest)
    grad_ada = ein("id,ic->dc", act_all, dmod_all)
    grad_ada_bias = jnp.sum(dmod_all.astype(f32), axis=0)
    return (
        result,
        d_tokens,
        grad_table,
        grad_ada,
        grad_ada_bias,
        grad_qkv,
        grad_q_bias,
        grad_v_bias,
        grad_scale,
        grad_proj,
        grad_proj_bias,
        grad_fc1,
        grad_fc1_bias,
        grad_fc2,
        grad_fc2_bias,
    )


def solution(mesh):
    return jax.shard_map(
        per_device,
        mesh=mesh,
        in_specs=(
            P("dp", None),
            P("dp", None),
            P(),
            P("dp", None),
            P(None, "tensor"),
            P(None, "tensor"),
            P("tensor"),
            P(None, None, "tensor"),
            P("tensor"),
            P("tensor"),
            P("tensor"),
            P("tensor", None),
            P(),
            P(None, "tensor"),
            P("tensor"),
            P("tensor", None),
            P(),
        ),
        out_specs=(
            P("dp", None),
            P("dp", None),
            P(None, "tensor"),
            P(None, "tensor"),
            P("tensor"),
            P(None, None, "tensor"),
            P("tensor"),
            P("tensor"),
            P("tensor"),
            P("tensor", None),
            P(),
            P(None, "tensor"),
            P("tensor"),
            P("tensor", None),
            P(),
        ),
        check_vma=False,
    )
```
